32 devices in a mesh: groups: 2 (over x), expert: 8 (over z, y), section: 2 (over core).
Axes of the slice: x: 2, y: 2, z: 4, core: 2. Of those that a mesh axis runs over, the one named last changes fastest.
Arguments:
- states: bfloat16 [2, 4096, 2048], P('section', ('groups', 'expert')), parts along dimension 1, may hold values from -6 to 6
- k_cache: bfloat16 [2, 1024, 4, 128], P('section', 'groups'), parts along dimension 1, may hold values from -600 to 600, as said below
- v_cache: bfloat16 [2, 1024, 4, 128], P('section', 'groups'), parts along dimension 1, may hold values from -6 to 6
- cache_len: int32 [2, 2], P('section', 'groups'), parts along dimension 1, may hold values from 256 to 512
- expert_ids: int32 [2, 4096, 2], P('section', ('groups', 'expert')), parts along dimension 1, may hold values from 0 to 3, all different within a row
- attn_gain: bfloat16 [2, 2048], P('section'), may hold values from 0.099609375 to 1.8984375
- moe_gain: bfloat16 [2, 2048], P('section'), may hold values from 0.099609375 to 1.8984375
- w_query: bfloat16 [2, 2048, 2048], P('section', None, 'expert'), may hold values from -0.125 to 0.125
- w_key: bfloat16 [2, 2048, 512], P('section', 'expert'), may hold values from -0.125 to 0.125
- w_value: bfloat16 [2, 2048, 512], P('section', 'expert'), may hold values from -0.125 to 0.125
- w_out: bfloat16 [2, 2048, 2048], P('section', 'expert'), may hold values from -0.125 to 0.125
- w_router: bfloat16 [2, 2048, 4], P('section'), may hold values from -0.5 to 0.5
- w_gate: bfloat16 [2, 8, 2048, 3584], P('section', 'expert'), may hold values from -0.125 to 0.125
- w_up: bfloat16 [2, 8, 2048, 3584], P('section', 'expert'), may hold values from -0.125 to 0.125
- w_down: bfloat16 [2, 8, 3584, 2048], P('section', 'expert'), may hold values from -0.0625 to 0.0625
Outputs:
- next_states: bfloat16 [2, 4096, 2048], P('section', ('groups', 'expert')), parts along dimension 1
The draws below stay inside these ranges and needn't reach their ends.
There are 2 independent parts, one for each index of `groups`. The reference program is written for one: setup_inputs(seed, part) draws one part's arguments, and reference() takes and returns one part's arrays. A program takes and returns all parts, laid end to end along the dimension named above; an argument that names none is the same for every part. Nothing has to cross between parts.
Inputs may be any that keep to these rules, and one draw needn't show every extreme that they name: `expert_ids`: the 2 experts of a token differ. `k_cache`: keys already rotated to their positions.
All inputs are finite; a program needn't handle non-finite values.
Results may differ from the reference program's by a relative error of at most 0.018.
Values may be sent and summed in bfloat16 or wider, within the bound.
No kernel may reach another device: no remote copies, remote signals or barrier semaphores. Data moves between devices by JAX's collectives and lax.ppermute only.
A program may use at most 192 MiB of HBM per device.

```python
import math
import jax
import jax.numpy as jnp
from jax import lax

D = 2048
HEADS = 16
HD = 128
KVH = 4
EXPERTS = 4
FF = 7168
TOP = 2
SPAN = 2048
CACHE = 512
ROWS = 256
SPLITS = 2
FF_DEV = 3584
HDEV = 2
CAP = 128
N_EXPERT = 8
N_SECTION = 2


def draw_k_cache(key, part):
    base = jnp.clip(jax.random.normal(key, (N_SECTION, CACHE, KVH, HD), jnp.float32), -6.0, 6.0)
    return base.astype(jnp.bfloat16)


def steps_of(stream_key, dims, cuts, least, largest):
    def one(axis_at, blocks):
        heights = jax.random.uniform(jax.random.fold_in(jax.random.fold_in(stream_key, 6), axis_at), (blocks,), jnp.float32, least / len(cuts), largest / len(cuts))
        return jnp.repeat(jnp.exp(heights), dims[axis_at] // blocks).reshape((-1,) + (1,) * (len(dims) - axis_at - 1))

    loudness = one(*cuts[0])
    for cut in cuts[1:]:
        loudness = loudness * one(*cut)
    return loudness


def picks_of(own_key, rows, number_of, top, lift):
    sequence = jax.random.permutation(jax.random.fold_in(own_key, 1), number_of)
    boost = sequence
    for power in range(3):
        boost = boost * boost // number_of
    boost = boost * lift // number_of
    lots = jax.random.randint(jax.random.fold_in(own_key, 2), (rows, number_of), 0, 4096) + boost
    sure = jax.random.permutation(jax.random.fold_in(own_key, 3), rows)[jnp.arange(number_of) % rows]
    lots = jnp.where(jnp.arange(rows)[:, None] == sure[None, :], 1 << 14, lots)
    score = lots * number_of + jnp.arange(number_of)
    return lax.top_k(score.astype(jnp.int32), top)[1].astype(jnp.int32)


def noise(rng, shape, deviation, reach, cuts=(), kind=jnp.bfloat16):
    drawn = deviation * jax.random.normal(rng, shape, jnp.float32)
    if cuts:
        drawn = drawn * steps_of(rng, shape, cuts, -0.22, 0.18)
    return jnp.clip(drawn, -reach, reach).astype(kind)


def setup_inputs(seed: int = 0, part: int = 0) -> dict:
    splits = jax.random.split(jax.random.key(seed), 16)
    own_keys = jax.random.split(jax.random.fold_in(splits[15], part), 16)
    states = noise(own_keys[0], (N_SECTION, SPAN, D), 1.0, 6.0, ((0, 2), (1, 8)))
    k_cache = draw_k_cache(jax.random.fold_in(jax.random.fold_in(splits[15], part), 71), part)
    v_cache = noise(own_keys[2], (N_SECTION, CACHE, KVH, HD), 1.0, 6.0, ((0, 2),))
    cache_len = jax.random.randint(own_keys[3], (N_SECTION, 1), CACHE // 2, CACHE + 1).astype(jnp.int32)
    expert_ids = picks_of(own_keys[4], N_SECTION * SPAN, EXPERTS, TOP, 8192).reshape((N_SECTION, SPAN, TOP))
    attn_gain = jnp.clip(1.0 + 0.18 * jax.random.normal(splits[5], (N_SECTION, D), jnp.float32), 0.099609375, 1.8984375).astype(jnp.bfloat16)
    moe_gain = jnp.clip(1.0 + 0.18 * jax.random.normal(splits[6], (N_SECTION, D), jnp.float32), 0.099609375, 1.8984375).astype(jnp.bfloat16)
    w_query = noise(splits[7], (N_SECTION, D, HEADS * HD), D ** -0.5, 0.125, ((0, 2), (2, 8)))
    w_key = noise(splits[8], (N_SECTION, D, KVH * HD), D ** -0.5, 0.125, ((0, 2), (1, 8)))
    w_value = noise(splits[9], (N_SECTION, D, KVH * HD), D ** -0.5, 0.125, ((0, 2), (1, 8)))
    w_out = noise(splits[10], (N_SECTION, HEADS * HD, D), (HEADS * HD) ** -0.5, 0.125, ((0, 2), (1, 8)))
    w_router = noise(splits[11], (N_SECTION, D, EXPERTS), (D // 16) ** -0.5, 0.5, ((0, 2),))
    w_gate = noise(splits[12], (N_SECTION, N_EXPERT, D, FF_DEV), D ** -0.5, 0.125, ((0, 2), (1, 8)))
    w_up = noise(splits[13], (N_SECTION, N_EXPERT, D, FF_DEV), D ** -0.5, 0.125, ((0, 2), (1, 8)))
    w_down = noise(splits[14], (N_SECTION, N_EXPERT, FF_DEV, D), FF ** -0.5, 0.0625, ((0, 2), (1, 8)))
    return {"states": states, "k_cache": k_cache, "v_cache": v_cache, "cache_len": cache_len, "expert_ids": expert_ids, "attn_gain": attn_gain, "moe_gain": moe_gain, "w_query": w_query, "w_key": w_key, "w_value": w_value, "w_out": w_out, "w_router": w_router, "w_gate": w_gate, "w_up": w_up, "w_down": w_down}


EPSILON = 1e-05
ROPE_BASE = 1000000.0

def normalize(inputs, gain_vec):
    values = inputs.astype(jnp.float32)
    return values * lax.rsqrt(lax.optimization_barrier(jnp.mean(values * values, axis=-1, keepdims=True)) + EPSILON) * gain_vec.astype(jnp.float32)

def rotate(tensor, positions):
    width_all = tensor.shape[-1]
    half_dim = width_all // 2
    frequency = ROPE_BASE ** (-(jnp.arange(half_dim, dtype=jnp.float32) * 2.0 / width_all))
    angles = positions[:, None] * frequency[None, :]
    cosine = jnp.cos(angles)[:, None, :]
    sine_part = jnp.sin(angles)[:, None, :]
    front_part = tensor[..., :half_dim]
    back_part = tensor[..., half_dim:]
    return jnp.concatenate([front_part * cosine - back_part * sine_part, back_part * cosine + front_part * sine_part], axis=-1)

def route_slots(ids, expert_count, capacity):
    hit_mask = (ids[..., None] == jnp.arange(expert_count, dtype=jnp.int32)).astype(jnp.int32).sum(axis=-2).astype(jnp.int32)
    before = (jnp.cumsum(hit_mask, axis=-2) - hit_mask).astype(jnp.int32)
    slot_pos = jnp.take_along_axis(before, ids, axis=-1).astype(jnp.int32)
    return (slot_pos, slot_pos < capacity)

def expert_piece(rows_in, gate_w, up_w, down_w):
    gate_act = jnp.dot(rows_in, gate_w, preferred_element_type=jnp.float32)
    up_act = jnp.dot(rows_in, up_w, preferred_element_type=jnp.float32)
    hidden = (jax.nn.silu(gate_act) * up_act).astype(jnp.bfloat16)
    return jnp.dot(hidden, down_w, preferred_element_type=jnp.float32).astype(jnp.bfloat16)

def layer(section_idx, states, k_cache, v_cache, cache_len, expert_ids, attn_gain, moe_gain, w_query, w_key, w_value, w_out, w_router, w_gate, w_up, w_down):
    inputs = states[section_idx]
    normed = normalize(inputs, attn_gain[section_idx]).astype(jnp.bfloat16)
    start_at = cache_len[section_idx, 0]
    positions = (start_at + jnp.arange(SPAN, dtype=jnp.int32)).astype(jnp.float32)
    query = jnp.dot(normed, w_query[section_idx], preferred_element_type=jnp.float32).reshape(SPAN, HEADS, HD)
    query = rotate(query, positions).astype(jnp.bfloat16)
    key_new = jnp.dot(normed, w_key[section_idx], preferred_element_type=jnp.float32).reshape(SPAN, KVH, HD)
    key_new = rotate(key_new, positions).astype(jnp.bfloat16)
    value_new = jnp.dot(normed, w_value[section_idx], preferred_element_type=jnp.float32).reshape(SPAN, KVH, HD).astype(jnp.bfloat16)
    all_keys = jnp.concatenate([k_cache[section_idx], key_new], axis=0)
    all_values = jnp.concatenate([v_cache[section_idx], value_new], axis=0)
    key_pos = jnp.arange(CACHE + SPAN, dtype=jnp.int32)
    query_pos = jnp.arange(SPAN, dtype=jnp.int32)
    is_valid = jnp.where(key_pos[None, :] < CACHE, (key_pos < start_at)[None, :], key_pos[None, :] - CACHE <= query_pos[:, None])
    scale_by = 1.0 / math.sqrt(HD)

    def one_head(head_idx):
        shared = head_idx // (HEADS // KVH)
        query_head = lax.dynamic_index_in_dim(query, head_idx, 1, keepdims=False)
        key_head = lax.dynamic_index_in_dim(all_keys, shared, 1, keepdims=False)
        value_head = lax.dynamic_index_in_dim(all_values, shared, 1, keepdims=False)
        scores = jnp.dot(query_head, key_head.T, preferred_element_type=jnp.float32) * scale_by
        scores = jnp.where(is_valid, scores, -jnp.inf)
        top_score = lax.optimization_barrier(jnp.max(scores, axis=-1, keepdims=True))
        exp_scores = jnp.exp(scores - top_score)
        attn_probs = (exp_scores / lax.optimization_barrier(jnp.sum(exp_scores, axis=-1, keepdims=True))).astype(jnp.bfloat16)
        return jnp.dot(attn_probs, value_head, preferred_element_type=jnp.float32).astype(jnp.bfloat16)
    attended = lax.map(one_head, jnp.arange(HEADS, dtype=jnp.int32))
    grouped = attended.reshape(N_EXPERT, HDEV, SPAN, HD).transpose(0, 2, 1, 3).reshape(N_EXPERT, SPAN, HDEV * HD)
    out_groups = w_out[section_idx].reshape(N_EXPERT, HDEV * HD, D)

    def add_group(total, pair):
        term_part = jnp.dot(pair[0], pair[1], preferred_element_type=jnp.float32).astype(jnp.bfloat16)
        term_part = lax.optimization_barrier(term_part)
        return (total + term_part.astype(jnp.float32), None)
    attn_sum, unused = lax.scan(add_group, jnp.zeros((SPAN, D), jnp.float32), (grouped, out_groups))
    mixed = inputs.astype(jnp.float32) + attn_sum
    moe_in = normalize(mixed, moe_gain[section_idx]).astype(jnp.bfloat16)
    ids = expert_ids[section_idx]
    slot_pos, is_kept = route_slots(ids.reshape(N_EXPERT, ROWS, TOP), EXPERTS, CAP)
    slot_pos = slot_pos.reshape(SPAN, TOP)
    is_kept = is_kept.reshape(SPAN, TOP)
    block_idx = (jnp.arange(SPAN, dtype=jnp.int32) // ROWS)[:, None]
    target = jnp.where(is_kept, (block_idx * EXPERTS + ids) * CAP + slot_pos, N_EXPERT * EXPERTS * CAP).astype(jnp.int32)
    buffer = jnp.zeros((N_EXPERT * EXPERTS * CAP, D), jnp.bfloat16)
    buffer = buffer.at[target.reshape(-1)].set(jnp.repeat(moe_in, TOP, axis=0), mode='drop')
    buffer = buffer.reshape(N_EXPERT, EXPERTS, CAP, D)

    def one_piece(device):
        owner = device // SPLITS
        rows_in = lax.dynamic_index_in_dim(buffer, owner, 1, keepdims=False).reshape(N_EXPERT * CAP, D)
        return expert_piece(rows_in, lax.dynamic_index_in_dim(w_gate[section_idx], device, 0, keepdims=False), lax.dynamic_index_in_dim(w_up[section_idx], device, 0, keepdims=False), lax.dynamic_index_in_dim(w_down[section_idx], device, 0, keepdims=False))
    pieces = lax.map(one_piece, jnp.arange(N_EXPERT, dtype=jnp.int32))
    pieces = lax.optimization_barrier(pieces)
    results = pieces.astype(jnp.float32).reshape(EXPERTS, SPLITS, N_EXPERT * CAP, D).sum(axis=1).reshape(EXPERTS * N_EXPERT * CAP, D)
    results = jnp.concatenate([results, jnp.zeros((1, D), jnp.float32)], axis=0)
    where_from = jnp.where(is_kept, ids * (N_EXPERT * CAP) + block_idx * CAP + slot_pos, EXPERTS * N_EXPERT * CAP).astype(jnp.int32)
    logits = jnp.dot(moe_in, w_router[section_idx], preferred_element_type=jnp.float32)
    picked = jnp.take_along_axis(logits, ids, axis=1)
    gate_mix = jnp.stack([jax.nn.sigmoid(picked[:, 0] - picked[:, 1]), jax.nn.sigmoid(picked[:, 1] - picked[:, 0])], axis=1)
    moe_out = lax.optimization_barrier(jnp.sum(gate_mix[:, :, None] * results[where_from], axis=1))
    return (mixed + moe_out).astype(jnp.bfloat16)

def reference(states, k_cache, v_cache, cache_len, expert_ids, attn_gain, moe_gain, w_query, w_key, w_value, w_out, w_router, w_gate, w_up, w_down):
    finished = []
    for section_idx in range(N_SECTION):
        finished.append(layer(section_idx, states, k_cache, v_cache, cache_len, expert_ids, attn_gain, moe_gain, w_query, w_key, w_value, w_out, w_router, w_gate, w_up, w_down))
    return jnp.roll(jnp.stack(finished, axis=0), 1, axis=0)
```

```python
import functools
import math

import jax
import jax.numpy as jnp
from jax import lax
from jax.experimental import pallas as pl
from jax.experimental.pallas import tpu as pltpu
from jax.sharding import PartitionSpec as P

EPSILON = 1e-05
ROPE_BASE = 1000000.0
NEG = -1e30


def shifted(shard, axis, by):
    size = lax.axis_size(axis)
    return lax.ppermute(shard, axis, [(i, (i + by) % size) for i in range(size)])


def outer_shift(shard, outer, inner, by):
    pairs = [
        (h * inner + l, ((h + by) % outer) * inner + l) for h in range(outer) for l in range(inner)
    ]
    return lax.ppermute(shard, "expert", pairs)


def inner_shift(shard, outer, inner, by):
    pairs = [
        (h * inner + l, h * inner + (l + by) % inner) for h in range(outer) for l in range(inner)
    ]
    return lax.ppermute(shard, "expert", pairs)


def normalize(inputs, gain_vec):
    values = inputs.astype(jnp.float32)
    return (
        values
        * lax.rsqrt(jnp.mean(values * values, axis=-1, keepdims=True) + EPSILON)
        * gain_vec.astype(jnp.float32)
    )


def rope_tables(positions, head_dim):
    half_dim = head_dim // 2
    frequency = ROPE_BASE ** (-(jnp.arange(half_dim, dtype=jnp.float32) * 2.0 / head_dim))
    angles = positions[:, None] * frequency[None, :]
    cosine, sine = jnp.cos(angles), jnp.sin(angles)
    return jnp.concatenate([cosine, cosine], -1), jnp.concatenate([-sine, sine], -1)


def rotate(tensor, cosine, sine):
    head_dim = cosine.shape[1]
    parts = []
    for at in range(0, tensor.shape[1], head_dim):
        head = tensor[:, at : at + head_dim]
        swapped = jnp.concatenate([head[:, head_dim // 2 :], head[:, : head_dim // 2]], axis=1)
        parts.append(head * cosine + swapped * sine)
    return jnp.concatenate(parts, axis=1) if len(parts) > 1 else parts[0]


def attend_kernel(where_ref, q_ref, kc_ref, vc_ref, kv_ref, o_ref, acc, top, den, *, outer, inner, heads, scale):
    rows = q_ref.shape[0]
    hd = kc_ref.shape[1]
    start_at, block, my_outer, my_inner = where_ref[0], where_ref[1], where_ref[2], where_ref[3]
    dims_nt = (((1,), (1,)), ((), ()))
    dims_tn = (((0,), (0,)), ((), ()))

    def step(keys, values, mask, first):
        for h in range(heads):
            query = q_ref[:, h * hd : (h + 1) * hd]
            s = lax.dot_general(keys, query, dims_nt, preferred_element_type=jnp.float32) * scale
            if mask is not None:
                s = jnp.where(mask, s, NEG)
            peak = jnp.max(s, axis=0, keepdims=True)
            if first:
                new_top = peak
            else:
                old_top = top[h : h + 1, :]
                new_top = jnp.maximum(old_top, peak)
            p = jnp.exp2(s - new_top)
            total = jnp.sum(p, axis=0, keepdims=True)
            part = lax.dot_general(
                values, p.astype(jnp.bfloat16), dims_tn, preferred_element_type=jnp.float32
            )
            if first:
                den[h : h + 1, :] = total
                acc[h] = part
            else:
                fade = jnp.exp2(old_top - new_top)
                den[h : h + 1, :] = den[h : h + 1, :] * fade + total
                acc[h] = acc[h] * fade + part
            top[h : h + 1, :] = new_top

    def slot_of(j):
        back = lax.rem(my_outer - lax.div(j, inner) + outer, outer)
        side = lax.rem(my_inner - lax.rem(j, inner) + inner, inner)
        return back * inner + side

    key_at = lax.broadcasted_iota(jnp.int32, (rows, rows), 0)
    query_at = lax.broadcasted_iota(jnp.int32, (rows, rows), 1)
    own = slot_of(block)
    step(kv_ref[own, :, :hd], kv_ref[own, :, hd:], key_at <= query_at, True)
    cache = kc_ref.shape[0]
    cache_at = lax.broadcasted_iota(jnp.int32, (cache, rows), 0)
    step(kc_ref[...], vc_ref[...], cache_at < start_at, False)

    def body(j, carry):
        at = slot_of(j)
        step(kv_ref[at, :, :hd], kv_ref[at, :, hd:], None, False)
        return carry

    lax.fori_loop(0, block, body, 0)
    for h in range(heads):
        done = acc[h] / den[h : h + 1, :]
        o_ref[:, h * hd : (h + 1) * hd] = done.T.astype(o_ref.dtype)


def attend(where, query, keys_cached, values_cached, kv_new, outer, inner):
    rows, width = query.shape
    hd = keys_cached.shape[1]
    heads = width // hd
    vmem = pl.BlockSpec(memory_space=pltpu.VMEM)
    return pl.pallas_call(
        functools.partial(
            attend_kernel, outer=outer, inner=inner, heads=heads, scale=math.log2(math.e) / math.sqrt(hd)
        ),
        out_shape=jax.ShapeDtypeStruct((rows, width), jnp.bfloat16),
        in_specs=[pl.BlockSpec(memory_space=pltpu.SMEM), vmem, vmem, vmem, vmem],
        out_specs=vmem,
        scratch_shapes=[
            pltpu.VMEM((heads, hd, rows), jnp.float32),
            pltpu.VMEM((max(heads, 8), rows), jnp.float32),
            pltpu.VMEM((max(heads, 8), rows), jnp.float32),
        ],
        compiler_params=pltpu.CompilerParams(vmem_limit_bytes=24 * 2**20),
        cost_estimate=pl.CostEstimate(
            flops=4 * rows * width * (outer * inner * rows // 2), transcendentals=0, bytes_accessed=2**22
        ),
        name="attend",
    )(where, query, keys_cached, values_cached, kv_new)


def expert_kernel(*refs, pieces):
    ins, (gate_ref, up_ref, down_ref) = refs[:pieces], refs[pieces : pieces + 3]
    outs, (rows_in, acc) = refs[pieces + 3 : 2 * pieces + 3], refs[2 * pieces + 3 :]
    at, steps = pl.program_id(0), pl.num_programs(0)
    each = ins[0].shape[0]

    @pl.when(at == 0)
    def _():
        for i, ref in enumerate(ins):
            rows_in[i * each : (i + 1) * each, :] = ref[...]

    x = rows_in[...]
    gate = jnp.dot(x, gate_ref[...], preferred_element_type=jnp.float32)
    up = jnp.dot(x, up_ref[...], preferred_element_type=jnp.float32)
    hidden = (gate * (1.0 / (1.0 + jnp.exp(-gate))) * up).astype(jnp.bfloat16)
    part = jnp.dot(hidden, down_ref[...], preferred_element_type=jnp.float32)

    @pl.when(at == 0)
    def _():
        acc[...] = part

    @pl.when(jnp.logical_and(at > 0, at < steps - 1))
    def _():
        acc[...] += part

    @pl.when(at == steps - 1)
    def _():
        total = (acc[...] + part).astype(jnp.bfloat16)
        for i, ref in enumerate(outs):
            ref[...] = total[i * each : (i + 1) * each, :]


def expert_rows(blocks, gate_w, up_w, down_w, tile=512):
    each, width = blocks[0].shape
    hidden = gate_w.shape[1]
    while hidden % tile:
        tile //= 2
    count = len(blocks)
    rows = each * count
    whole = pl.BlockSpec((each, width), lambda i: (0, 0))
    return pl.pallas_call(
        functools.partial(expert_kernel, pieces=count),
        grid=(hidden // tile,),
        out_shape=[jax.ShapeDtypeStruct((each, width), jnp.bfloat16)] * count,
        in_specs=[whole] * count
        + [
            pl.BlockSpec((width, tile), lambda i: (0, i)),
            pl.BlockSpec((width, tile), lambda i: (0, i)),
            pl.BlockSpec((tile, width), lambda i: (i, 0)),
        ],
        out_specs=[whole] * count,
        scratch_shapes=[pltpu.VMEM((rows, width), jnp.bfloat16), pltpu.VMEM((rows, width), jnp.float32)],
        compiler_params=pltpu.CompilerParams(
            dimension_semantics=("arbitrary",), vmem_limit_bytes=48 * 2**20
        ),
        cost_estimate=pl.CostEstimate(
            flops=6 * rows * width * hidden, transcendentals=rows * hidden, bytes_accessed=6 * width * hidden
        ),
        name="expert_rows",
    )(*blocks, gate_w, up_w, down_w)


def body(
    states,
    k_cache,
    v_cache,
    cache_len,
    expert_ids,
    attn_gain,
    moe_gain,
    w_query,
    w_key,
    w_value,
    w_out,
    w_router,
    w_gate,
    w_up,
    w_down,
):
    me = lax.axis_index("expert")
    devices = lax.axis_size("expert")
    x_rows = states[0]
    row_count, width_all = x_rows.shape
    kv_heads = k_cache.shape[2]
    head_dim = k_cache.shape[3]
    outer, inner = kv_heads, devices // kv_heads
    hi, lo = me // inner, me % inner
    start_at = cache_len[0, 0]

    normed = [normalize(x_rows, attn_gain[0]).astype(jnp.bfloat16)]
    kv_parts = []
    for k in range(outer):
        col = ((hi + k) % outer) * head_dim
        part = jnp.concatenate(
            [
                lax.dynamic_slice_in_dim(w_key[0], col, head_dim, 1),
                lax.dynamic_slice_in_dim(w_value[0], col, head_dim, 1),
            ],
            axis=1,
        )
        kv_parts.append(outer_shift(part, outer, inner, k) if k else part)
    for k in range(1, outer):
        normed.append(outer_shift(normed[-1], outer, inner, 1))
    kv_plane = [jnp.stack(kv_parts)]
    query_w = [w_query[0]]
    for j in range(1, inner):
        kv_plane.append(inner_shift(kv_plane[-1], outer, inner, 1))
        query_w.append(inner_shift(query_w[-1], outer, inner, 1))
    kv_plane = jnp.stack(kv_plane)
    kv_w = jnp.concatenate(
        [
            lax.dynamic_slice(
                kv_plane,
                ((lo - l) % inner, (hi - h) % outer, 0, 0),
                (1, 1) + kv_plane.shape[2:],
            )[0, 0]
            for h in range(outer)
            for l in range(inner)
        ],
        axis=0,
    )
    projection = jnp.concatenate(query_w + [kv_w], axis=1)
    query_width = projection.shape[1] - 2 * head_dim

    queries, kv_own, blocks = [], [], []
    for k in range(outer):
        block = ((hi - k) % outer) * inner + lo
        blocks.append(block)
        positions = (
            start_at + block * row_count + jnp.arange(row_count, dtype=jnp.int32)
        ).astype(jnp.float32)
        cosine, sine = rope_tables(positions, head_dim)
        mapped = jnp.dot(normed[k], projection, preferred_element_type=jnp.float32)
        turned = rotate(mapped[:, : query_width + head_dim], cosine, sine).astype(jnp.bfloat16)
        queries.append(turned[:, :query_width])
        kv_own.append(
            jnp.concatenate(
                [turned[:, query_width:], mapped[:, query_width + head_dim :].astype(jnp.bfloat16)], axis=1
            )
        )
    kv_all = [[kv] for kv in kv_own]
    for k in range(outer):
        for j in range(1, inner):
            kv_all[k].append(inner_shift(kv_all[k][-1], outer, inner, 1))
    kv_new = jnp.stack([kv for group in kv_all for kv in group])
    keys_cached = lax.dynamic_index_in_dim(k_cache[0], hi, 1, keepdims=False)
    values_cached = lax.dynamic_index_in_dim(v_cache[0], hi, 1, keepdims=False)

    attended = []
    for k in range(outer):
        where = jnp.stack([start_at, blocks[k], hi, lo]).astype(jnp.int32)
        part = attend(where, queries[k], keys_cached, values_cached, kv_new, outer, inner)
        attended.append(outer_shift(part, outer, inner, -k) if k else part)
    out_w = lax.all_gather(w_out[0], "expert", axis=0, tiled=True)
    out_w = out_w.reshape(outer, inner, w_out.shape[1], width_all)
    columns = []
    for h in range(outer):
        whole = lax.dynamic_index_in_dim(jnp.stack(attended), (h - hi) % outer, 0, keepdims=False)
        whole = whole.reshape(row_count, inner, -1)
        for l in range(inner):
            columns.append(lax.dynamic_index_in_dim(whole, (lo - l) % inner, 1, keepdims=False))
    attn_rows = jnp.dot(
        jnp.concatenate(columns, axis=1),
        out_w.reshape(-1, width_all),
        preferred_element_type=jnp.float32,
    )

    expert_count = w_router.shape[2]
    e_outer, e_inner = expert_count, devices // expert_count
    e_hi = me // e_inner
    top_k = expert_ids.shape[2]
    capacity = row_count * top_k // expert_count
    ids_rows = expert_ids[0]
    names = jnp.arange(expert_count, dtype=jnp.int32)
    hits = (ids_rows[:, :, None] == names).astype(jnp.float32)
    hit_mask = hits.sum(axis=1)
    earlier = (
        jnp.arange(row_count)[:, None] > jnp.arange(row_count)[None, :]
    ).astype(jnp.bfloat16)
    before = jnp.dot(earlier, hit_mask.astype(jnp.bfloat16), preferred_element_type=jnp.float32)
    slot = (before[:, None, :] * hits).sum(axis=-1).astype(jnp.int32)
    relative = (ids_rows - e_hi) % e_outer
    target = jnp.where(slot < capacity, relative * capacity + slot, -1)
    places = jnp.arange(expert_count * capacity, dtype=jnp.int32)
    chosen = (target[:, :, None] == places).astype(jnp.float32)
    select = chosen.sum(axis=1).astype(jnp.bfloat16)

    h_rows = x_rows.astype(jnp.float32) + attn_rows
    moe_rows = normalize(h_rows, moe_gain[0]).astype(jnp.bfloat16)
    packed = lax.dot_general(
        select, moe_rows, (((0,), (0,)), ((), ())), preferred_element_type=jnp.float32
    ).astype(jnp.bfloat16)
    packed = packed.reshape(e_outer, capacity, width_all)
    arrived = []
    for k in range(e_outer):
        rows = outer_shift(packed[k], e_outer, e_inner, k) if k else packed[0]
        group = [rows]
        for j in range(1, e_inner):
            group.append(inner_shift(group[-1], e_outer, e_inner, 1))
        arrived.append(group)
    logits = jnp.dot(moe_rows, w_router[0], preferred_element_type=jnp.float32)
    picked = (logits[:, None, :] * hits).sum(axis=-1)
    gate_mix = jnp.stack(
        [jax.nn.sigmoid(picked[:, 0] - picked[:, 1]), jax.nn.sigmoid(picked[:, 1] - picked[:, 0])],
        axis=1,
    )
    weights = (chosen * gate_mix[:, :, None]).sum(axis=1)
    weights_hi = weights.astype(jnp.bfloat16)
    weights_lo = (weights - weights_hi.astype(jnp.float32)).astype(jnp.bfloat16)

    merged = [None] * e_outer
    halves = max(1, e_outer // 2)
    for chunk in [list(range(c, c + halves)) for c in range(0, e_outer, halves)]:
        flat = [rows for k in chunk for rows in arrived[k]]
        results = expert_rows(flat, w_gate[0, 0], w_up[0, 0], w_down[0, 0])
        for i, k in enumerate(chunk):
            group = results[i * e_inner : (i + 1) * e_inner]
            total = group[0].astype(jnp.float32)
            for j in range(1, e_inner):
                total = total + inner_shift(group[j], e_outer, e_inner, -j).astype(jnp.float32)
            total = total.astype(jnp.bfloat16)
            merged[k] = outer_shift(total, e_outer, e_inner, -k) if k else total
    moe_in = jnp.concatenate(merged, axis=0)
    moe_out = jnp.dot(weights_hi, moe_in, preferred_element_type=jnp.float32) + jnp.dot(
        weights_lo, moe_in, preferred_element_type=jnp.float32
    )
    layer_rows = (h_rows + moe_out).astype(jnp.bfloat16)
    passed = shifted(layer_rows, "section", 1)
    return passed[None]


def solution(mesh):
    in_specs = (
        P("section", ("groups", "expert"), None),
        P("section", "groups", None, None),
        P("section", "groups", None, None),
        P("section", "groups"),
        P("section", ("groups", "expert"), None),
        P("section", None),
        P("section", None),
        P("section", None, "expert"),
        P("section", "expert", None),
        P("section", "expert", None),
        P("section", "expert", None),
        P("section", None, None),
        P("section", "expert", None, None),
        P("section", "expert", None, None),
        P("section", "expert", None, None),
    )
    out_specs = P("section", ("groups", "expert"), None)
    return jax.shard_map(body, mesh=mesh, in_specs=in_specs, out_specs=out_specs, check_vma=False)
```
